32 devices in a mesh: row: 16 (over z, y, x), width: 2 (over core).
Axes of the slice: x: 2, y: 2, z: 4, core: 2. Of those that a mesh axis runs over, the one named last changes fastest.
Arguments:
- row_numbers: int32 [512, 2], P('row'), may hold values from 0 to 16383
- item_table: bfloat16 [16384, 64], P('row', 'width'), may hold values from -6 to 6
- dense_part: float32 [512, 64], P('row', 'width'), may hold values from -6 to 6
- small_ids: int32 [512], P('row'), may hold values from 0 to 31
- small_table: bfloat16 [32, 64], P('row', 'width'), may hold values from -6 to 6
Outputs:
- features: bfloat16 [512, 3, 64], P('row', None, 'width')
The draws below stay inside these ranges and needn't reach their ends.
All inputs are finite; a program needn't handle non-finite values.
Results may differ from the reference program's by a relative error of at most 0.0004.
Values may be sent and summed in bfloat16 or wider, within the bound.
A program may use at most 64 MiB of HBM per device.

```python
import math
import jax
import jax.numpy as jnp
import numpy as np

EXAMPLES = 512
FEATURES = 64
PICKS = 2
BIG_ROWS = 16384
SMALL_ROWS = 32


def set_ends(entries, stream_key, least, largest):
    spot = [jax.random.randint(jax.random.fold_in(stream_key, axis), (), 0, length) for axis, length in enumerate(entries.shape)]
    widest = entries.shape.index(max(entries.shape))
    neighbour = spot[:widest] + [(spot[widest] + 1) % entries.shape[widest]] + spot[widest + 1:]
    return entries.at[tuple(spot)].set(least).at[tuple(neighbour)].set(largest)


def levels(rng, dims, split, low, top_value):
    loudness, own = 1.0, jax.random.fold_in(rng, 6)
    for dim, blocks in split:
        heights = jnp.exp(jax.random.uniform(jax.random.fold_in(own, dim), (blocks,), jnp.float32, low / len(split), top_value / len(split)))
        loudness = loudness * jnp.repeat(heights, dims[dim] // blocks).reshape([-1 if axis == dim else 1 for axis in range(len(dims))])
    return loudness


def rank_table(count, lean):
    weights = [(1 << 20) // math.isqrt(grade ** lean) + 1 for grade in range(1, count + 1)]
    scale = 1 + sum(weights) // (1 << 30)
    return np.cumsum(np.array([max(1, weight // scale) for weight in weights]))


def ranked_ids(key, dims, number_of, lean):
    table = rank_table(number_of, lean)
    ticket = jax.random.randint(jax.random.fold_in(key, 1), dims, 0, int(table[number_of - 1]))
    standing = jnp.searchsorted(jnp.asarray(table, jnp.int32), ticket, side="right")
    return jax.random.permutation(jax.random.fold_in(key, 2), number_of)[standing].astype(jnp.int32)


def scatter_about(stream_key, extent, scale, limit, cuts=(), dtype=jnp.bfloat16):
    result = scale * jax.random.normal(stream_key, extent, jnp.float32)
    if cuts:
        result = result * levels(stream_key, extent, cuts, -0.22, 0.18)
    return jnp.clip(result, -limit, limit).astype(dtype)


def setup_inputs(seed: int = 0) -> dict:
    splits = jax.random.split(jax.random.key(seed), 6)
    row_numbers = set_ends(ranked_ids(splits[0], (EXAMPLES, PICKS), BIG_ROWS, 2), jax.random.fold_in(splits[0], 3), 0, BIG_ROWS - 1).astype(jnp.int32)
    item_table = scatter_about(splits[1], (BIG_ROWS, FEATURES), 1.0, 6.0, ((0, 16), (1, 2)))
    dense_part = scatter_about(splits[2], (EXAMPLES, FEATURES), 1.0, 6.0, ((0, 16), (1, 2)), jnp.float32)
    small_ids = set_ends(jax.random.randint(splits[3], (EXAMPLES,), 0, SMALL_ROWS), jax.random.fold_in(splits[3], 1), 0, SMALL_ROWS - 1).astype(jnp.int32)
    small_table = scatter_about(splits[4], (SMALL_ROWS, FEATURES), 1.0, 6.0, ((0, 16), (1, 2)))
    return {"row_numbers": row_numbers, "item_table": item_table, "dense_part": dense_part, "small_ids": small_ids, "small_table": small_table}


def reference(row_numbers, item_table, dense_part, small_ids, small_table):
    pooled = jnp.sum(item_table[row_numbers].astype(jnp.float32), axis=1) * PICKS ** -0.5
    small_rows = small_table[small_ids].astype(jnp.float32)
    features = jnp.stack([dense_part, pooled, small_rows], axis=1).astype(jnp.bfloat16)
    return features
```

```python
import functools

import jax
import jax.numpy as jnp
from jax import lax
from jax.experimental import pallas as pl
from jax.experimental.pallas import tpu as pltpu
from jax.sharding import PartitionSpec as P

MESH = pl.DeviceIdType.MESH


def near_size(count):
    return max(d for d in range(1, count + 1) if count % d == 0 and d * d <= count)


def target(place, step, count):
    return place ^ step if count & (count - 1) == 0 else (place + step) % count


def source(place, step, count):
    return place ^ step if count & (count - 1) == 0 else (place - step + count) % count


def kernel(
    near, far, scale,
    ids_hbm, table_hbm, dense_hbm, small_ids_hbm, small_hbm, out_ref,
    ids, tables, dense, small_ids, smalls, packed, arrived,
    local_sem, ids_out, ids_in, tab_out, tab_in, sm_out, sm_in, sf_out, sf_in, val_out, val_in,
):
    me = lax.axis_index("row")
    low, high = me % near, me // near
    picks, examples = ids.shape[1:]
    features, rows = tables.shape[1:]
    small_span = smalls.shape[2]

    def near_to(step):
        return {"row": high * near + target(low, step, near)}

    def far_to(step):
        return {"row": target(high, step, far) * near + low}

    def far_back(step):
        return {"row": source(high, step, far) * near + low}

    barrier = pltpu.get_barrier_semaphore()
    for step in range(1, far):
        pl.semaphore_signal(barrier, inc=1, device_id=far_to(step), device_id_type=MESH)
    for step in range(1, near):
        pl.semaphore_signal(barrier, inc=1, device_id=near_to(step), device_id_type=MESH)

    own = [
        pltpu.make_async_copy(src, dst, local_sem.at[i])
        for i, (src, dst) in enumerate(
            [
                (ids_hbm, ids.at[0]),
                (table_hbm, tables.at[0]),
                (small_hbm, smalls.at[0, 0]),
                (dense_hbm, dense),
                (small_ids_hbm, small_ids),
            ]
        )
    ]
    for copy in own:
        copy.start()

    def remote(src, dst, out_sem, in_sem, device):
        return pltpu.make_async_remote_copy(
            src_ref=src, dst_ref=dst, send_sem=out_sem, recv_sem=in_sem,
            device_id=device, device_id_type=MESH,
        )

    ids_copies = [
        remote(ids.at[0], ids.at[s], ids_out.at[s], ids_in.at[s], far_to(s)) for s in range(1, far)
    ]
    table_copies = [
        remote(tables.at[0], tables.at[s], tab_out.at[s], tab_in.at[s], near_to(s))
        for s in range(1, near)
    ]
    small_copies = [
        remote(smalls.at[0, 0], smalls.at[0, s], sm_out.at[s], sm_in.at[s], near_to(s))
        for s in range(1, near)
    ]
    small_far = [
        remote(smalls.at[0], smalls.at[s], sf_out.at[s], sf_in.at[s], far_to(s))
        for s in range(1, far)
    ]
    value_copies = [
        remote(packed.at[s], arrived.at[s], val_out.at[s], val_in.at[s], far_back(s))
        for s in range(1, far)
    ]

    own[0].wait()
    own[1].wait()
    own[2].wait()
    pl.semaphore_wait(barrier, far - 1 + near - 1)
    for copy in reversed(ids_copies):
        copy.start()
    for copy in small_copies:
        copy.start()
    for copy in reversed(table_copies):
        copy.start()

    own[3].wait()
    own[4].wait()
    out_ref[0] = dense[...].astype(out_ref.dtype)

    for copy in ids_copies:
        copy.wait_recv()
    wanted = jnp.concatenate([ids[s] for s in range(far)], axis=1)
    lanes = far * examples
    spot = lax.broadcasted_iota(jnp.int32, (rows, lanes), 0)

    def chosen(step):
        first = (high * near + source(low, step, near)) * rows
        hits = 0.0
        for pick in range(picks):
            hits = hits + jnp.where(spot == wanted[pick : pick + 1] - first, 1.0, 0.0)
        return hits.astype(tables.dtype)

    found = jnp.zeros((features, lanes), jnp.float32)
    for step in range(near):
        hits = chosen(step)
        if step:
            small_copies[step - 1].wait_recv()
            table_copies[step - 1].wait_recv()
        found = found + jnp.dot(tables[step], hits, preferred_element_type=jnp.float32)

    blocks = features // 8
    for step in reversed(range(far)):
        packed[step] = jnp.concatenate(
            [
                found[8 * b : 8 * b + 8, step * examples : (step + 1) * examples]
                for b in range(blocks)
            ],
            axis=1,
        )
        if step:
            value_copies[step - 1].start()
    for copy in reversed(small_far):
        copy.start()

    small_column = jnp.broadcast_to(small_ids[...], (8, examples)).T[:, 0:1]
    for copy in small_far:
        copy.wait_recv()
    rows_out = jnp.zeros((examples, features), jnp.float32)
    for far_step in range(far):
        for near_step in range(near):
            device = source(high, far_step, far) * near + source(low, near_step, near)
            part = smalls[far_step, near_step].astype(jnp.float32)
            for r in range(small_span):
                rows_out = jnp.where(
                    small_column == device * small_span + r, part[r : r + 1], rows_out
                )
    out_ref[2] = rows_out.astype(out_ref.dtype)

    total = packed[0]
    for step in range(1, far):
        value_copies[step - 1].wait_recv()
        total = total + arrived[step]
    total = total * scale
    pooled = jnp.concatenate(
        [total[:, b * examples : (b + 1) * examples] for b in range(blocks)], axis=0
    ).T
    out_ref[1] = pooled.astype(out_ref.dtype)

    for copy in ids_copies + table_copies + small_copies + small_far + value_copies:
        copy.wait_send()


def per_device(count, row_numbers, item_table, dense_part, small_ids, small_table):
    near = near_size(count)
    far = count // near
    examples, picks = row_numbers.shape
    rows, features = item_table.shape
    dma = pltpu.SemaphoreType.DMA
    out = pl.pallas_call(
        functools.partial(kernel, near, far, picks ** (-0.5)),
        out_shape=jax.ShapeDtypeStruct((3, examples, features), jnp.bfloat16),
        in_specs=[pl.BlockSpec(memory_space=pl.ANY)] * 5,
        out_specs=pl.BlockSpec(memory_space=pltpu.VMEM),
        scratch_shapes=[
            pltpu.VMEM((far, picks, examples), jnp.int32),
            pltpu.VMEM((near, features, rows), item_table.dtype),
            pltpu.VMEM(dense_part.shape, dense_part.dtype),
            pltpu.VMEM((1, examples), jnp.int32),
            pltpu.VMEM((far, near) + small_table.shape, small_table.dtype),
            pltpu.VMEM((far, 8, features // 8 * examples), jnp.float32),
            pltpu.VMEM((far, 8, features // 8 * examples), jnp.float32),
            dma((5,)),
            dma((far,)), dma((far,)),
            dma((near,)), dma((near,)),
            dma((near,)), dma((near,)),
            dma((far,)), dma((far,)),
            dma((far,)), dma((far,)),
        ],
        compiler_params=pltpu.CompilerParams(collective_id=0, has_side_effects=True),
    )(row_numbers.T, item_table.T, dense_part, small_ids[None, :], small_table)
    return jnp.transpose(out, (1, 0, 2))


def solution(mesh):
    placed = (P("row", None), P("row", "width"), P("row", "width"), P("row"), P("row", "width"))
    return jax.shard_map(
        functools.partial(per_device, mesh.shape["row"]),
        mesh=mesh, in_specs=placed, out_specs=P("row", None, "width"), check_vma=False,
    )
```
